512 devices in a mesh: groups: 2 (over y), dom: 32 (over z), tilt: 4 (over x), rep: 2 (over core).
Axes of the slice: x: 4, y: 2, z: 32, core: 2. Of those that a mesh axis runs over, the one named last changes fastest.
The devices are a block of a 4x8x32 slice.
Arguments:
- patches: bfloat16 [8, 4096, 128, 128], P(('groups', 'tilt'), 'dom'), parts along dimension 0, may hold values from -6 to 6
- slot_view: int32 [8, 4096, 1], P(('groups', 'tilt'), 'dom'), parts along dimension 0, may hold values from 0 to 127, as said below
- slot_tilt: int32 [8, 4096], P(('groups', 'tilt'), 'dom'), parts along dimension 0, may hold values from 0 to 9
- slot_pos: bfloat16 [2, 8, 4096], P(None, ('groups', 'tilt'), 'dom'), parts along dimension 1, may hold values from 0 to 1
- defocus: bfloat16 [8, 4096], P(('groups', 'tilt'), 'dom'), parts along dimension 0, may hold values from 1 to 3
- projections: bfloat16 [256, 40, 2, 128, 128], P(('groups', 'dom'), 'tilt', None, 'rep'), parts along dimension 0, may hold values from -6 to 6
- warp_grid: float32 [80, 2, 256], P(('groups', 'tilt')), parts along dimension 0, may hold values from -6 to 6
Outputs:
- slot_terms: float32 [3, 8, 4096], P(None, ('groups', 'tilt'), 'dom'), parts along dimension 1
- new_warp: float32 [80, 2, 256], P(('groups', 'tilt')), parts along dimension 0
The draws below stay inside these ranges and needn't reach their ends.
There are 2 independent parts, one for each index of `groups`. The reference program is written for one: setup_inputs(seed, part) draws one part's arguments, and reference() takes and returns one part's arrays. A program takes and returns all parts, laid end to end along the dimension named above; each array names one. Nothing has to cross between parts.
Inputs may be any that keep to these rules, and one draw needn't show every extreme that they name: `slot_view`: view v is owned by dom index v // 4. Among the 128 slots of one device (one tilt index and one dom index) at most 6 name views of any one owner, and in every such block some owner is named exactly 6 times.
All inputs are finite; a program needn't handle non-finite values.
Results may differ from the reference program's by a relative error of at most 0.0018.
Values may be sent and summed in bfloat16 or wider, within the bound.
No kernel may reach another device: no remote copies, remote signals or barrier semaphores. Data moves between devices by JAX's collectives and lax.ppermute only.
A program may use at most 64 MiB of HBM per device.

```python
import math
import jax
import jax.numpy as jnp
from jax import lax

PATCH = 128
GRID = 16
VIEW_DEV = 4
TILT_DEV = 10
SLOT_DEV = 128
VIEWS = 128
TILTS = 40
SLOTS = 4096
OWN_CAP = 6
NODES = 256
N_DOM = 32
N_TILT = 4


def draw_slot_view(key, part):
    block_total = N_TILT * N_DOM
    base_load = SLOT_DEV // N_DOM
    spare_load = OWN_CAP - base_load
    half_owners = N_DOM // 2
    hot_owner = jax.random.randint(jax.random.fold_in(key, 7), (), 0, N_DOM).astype(jnp.int32)

    def one_block(block_key):
        key_order, key_delta, key_shuffle, key_view = jax.random.split(block_key, 4)
        order = jax.random.permutation(key_order, N_DOM - 1).astype(jnp.int32)
        others = order + (order >= hot_owner).astype(jnp.int32)
        arrange = jnp.concatenate([hot_owner[None], others])
        delta = jax.random.randint(key_delta, (half_owners,), 0, spare_load + 1).astype(jnp.int32)
        delta = delta.at[0].set(spare_load)
        deltas = jnp.concatenate([delta, -delta])
        counts = jnp.zeros((N_DOM,), jnp.int32).at[arrange].set(base_load + deltas)
        ends = jnp.cumsum(counts)
        slot_iota = jnp.arange(SLOT_DEV, dtype=jnp.int32)
        owner = jnp.sum((ends[None, :] <= slot_iota[:, None]).astype(jnp.int32), axis=1)
        owner = owner[jax.random.permutation(key_shuffle, SLOT_DEV)]
        return owner * VIEW_DEV + jax.random.randint(key_view, (SLOT_DEV,), 0, VIEW_DEV).astype(jnp.int32)
    block_keys = jax.random.split(jax.random.fold_in(key, 3), block_total)
    views_all = jax.vmap(one_block)(block_keys)
    return views_all.reshape(N_TILT, SLOTS, 1).astype(jnp.int32)


def place_ends(array, stream_key, least, largest):
    longest = array.shape.index(max(array.shape))
    spots = []
    for shift in (0, 1):
        where = [jax.random.randint(jax.random.fold_in(stream_key, axis), (), 0, length) for axis, length in enumerate(array.shape)]
        where[longest] = (where[longest] + shift) % array.shape[longest]
        spots.append(tuple(where))
    return array.at[spots[0]].set(least).at[spots[1]].set(largest)


def levels(stream_key, extent, cuts, low, largest):
    def one(dim, parts):
        steps = jax.random.uniform(jax.random.fold_in(jax.random.fold_in(stream_key, 6), dim), (parts,), jnp.float32, low / len(cuts), largest / len(cuts))
        return jnp.repeat(jnp.exp(steps), extent[dim] // parts).reshape((-1,) + (1,) * (len(extent) - dim - 1))

    loudness = one(*cuts[0])
    for cut in cuts[1:]:
        loudness = loudness * one(*cut)
    return loudness


def gaussian(own_key, extent, scale, limit, shards=(), held_as=jnp.bfloat16):
    values = scale * jax.random.normal(own_key, extent, jnp.float32)
    if shards:
        values = values * levels(own_key, extent, shards, -0.22, 0.18)
    return jnp.clip(values, -limit, limit).astype(held_as)


def setup_inputs(seed: int = 0, part: int = 0) -> dict:
    splits = jax.random.split(jax.random.key(seed), 8)
    part_splits = jax.random.split(jax.random.fold_in(splits[7], part), 8)
    return {
        "patches": gaussian(part_splits[0], (N_TILT, SLOTS, PATCH, PATCH), 1.0, 6.0, ((0, 4), (1, 32))),
        "slot_view": draw_slot_view(jax.random.fold_in(jax.random.fold_in(splits[7], part), 71), part),
        "slot_tilt": place_ends(jax.random.randint(part_splits[2], (N_TILT, SLOTS), 0, TILT_DEV), jax.random.fold_in(part_splits[2], 1), 0, TILT_DEV - 1).astype(jnp.int32),
        "slot_pos": jnp.clip(1.0 * jax.random.uniform(part_splits[3], (2, N_TILT, SLOTS), jnp.float32) ** levels(part_splits[3], (2, N_TILT, SLOTS), ((1, 4), (2, 32)), -0.2, 0.2), 0.0, 1.0).astype(jnp.bfloat16),
        "defocus": jnp.clip(jnp.exp(math.log(3.0) - 1.0986123 * jax.random.uniform(part_splits[4], (N_TILT, SLOTS), jnp.float32) ** levels(part_splits[4], (N_TILT, SLOTS), ((0, 4), (1, 32)), -0.2, 0.2)), 1.0, 3.0).astype(jnp.bfloat16),
        "projections": gaussian(part_splits[5], (VIEWS, TILTS, 2, PATCH, PATCH), 1.0, 6.0, ((0, 32), (1, 4), (3, 2))),
        "warp_grid": gaussian(part_splits[6], (TILTS, 2, NODES), 1.5, 6.0, ((0, 4),), jnp.float32),
    }


AMPLITUDE = 0.07
TRUST_FLOOR = 0.02

def signed_freq(index, pixels):
    return jnp.where(index < pixels // 2, index, index - pixels).astype(jnp.float32)

def dft_tables(freq_rows, pixels):
    columns = jnp.arange(pixels, dtype=jnp.int32)
    table_scale = 1.0 / math.sqrt(pixels)
    turns_rows = (freq_rows[:, None] * columns[None, :] % pixels).astype(jnp.float32) * (2.0 * math.pi / pixels)
    turns_full = (columns[:, None] * columns[None, :] % pixels).astype(jnp.float32) * (2.0 * math.pi / pixels)
    row_table = jnp.concatenate([jnp.cos(turns_rows), jnp.sin(turns_rows)], axis=0) * table_scale
    col_table = jnp.concatenate([jnp.cos(turns_full), jnp.sin(turns_full)], axis=1) * table_scale
    return (row_table.astype(jnp.bfloat16), col_table.astype(jnp.bfloat16))

def node_weights(pos_x, pos_y, grid_side):
    knot_pos = jnp.arange(grid_side, dtype=jnp.int32).astype(jnp.float32)
    weight_x = jnp.maximum(0.0, 1.0 - jnp.abs(pos_x[:, None] * (grid_side - 1) - knot_pos[None, :]))
    weight_y = jnp.maximum(0.0, 1.0 - jnp.abs(pos_y[:, None] * (grid_side - 1) - knot_pos[None, :]))
    return (weight_y[:, :, None] * weight_x[:, None, :]).reshape(pos_x.shape[0], grid_side * grid_side)

def spectral_terms(spectrum, ref_blk, focus_blk, shift_blk, freq_rows, pixels):
    row_total = freq_rows.shape[0]
    v_one_cos = spectrum[:, :row_total, :pixels]
    v_one_sin = spectrum[:, :row_total, pixels:]
    v_two_cos = spectrum[:, row_total:, :pixels]
    v_two_sin = spectrum[:, row_total:, pixels:]
    real_part = v_one_cos - v_two_sin
    imag_part = -(v_one_sin + v_two_cos)
    freq_y = signed_freq(freq_rows, pixels)[None, :, None]
    freq_x = signed_freq(jnp.arange(pixels, dtype=jnp.int32), pixels)[None, None, :]
    nyquist = pixels / 2.0
    radius = (freq_y * freq_y + freq_x * freq_x) / (nyquist * nyquist)
    aberration = math.pi * focus_blk[:, None, None] * radius
    contrast = -(math.sqrt(1.0 - AMPLITUDE * AMPLITUDE) * jnp.sin(aberration) + AMPLITUDE * jnp.cos(aberration))
    phase_angle = 2.0 * math.pi / pixels * (freq_x * shift_blk[:, 0, None, None] + freq_y * shift_blk[:, 1, None, None])
    cosine = jnp.cos(phase_angle)
    sine_part = jnp.sin(phase_angle)
    ref_real = ref_blk[:, 0].astype(jnp.float32)
    ref_imag = ref_blk[:, 1].astype(jnp.float32)
    model_real = contrast * (ref_real * cosine + ref_imag * sine_part)
    model_imag = contrast * (ref_imag * cosine - ref_real * sine_part)
    diff_real = real_part - model_real
    diff_imag = imag_part - model_imag
    inverse_area = 1.0 / (pixels * pixels)
    energy = lax.optimization_barrier(jnp.sum(diff_real * diff_real + diff_imag * diff_imag, axis=(1, 2))) * inverse_area
    cross_term = diff_imag * model_real - diff_real * model_imag
    grad_x = 2.0 * inverse_area * lax.optimization_barrier(jnp.sum(2.0 * math.pi / pixels * freq_x * cross_term, axis=(1, 2)))
    grad_y = 2.0 * inverse_area * lax.optimization_barrier(jnp.sum(2.0 * math.pi / pixels * freq_y * cross_term, axis=(1, 2)))
    return jnp.stack([energy, grad_x, grad_y], axis=1)

def reference(patches, slot_view, slot_tilt, slot_pos, defocus, projections, warp_grid):
    slot_total = N_TILT * SLOTS
    tilt_index = (jnp.arange(N_TILT, dtype=jnp.int32)[:, None] * TILT_DEV + slot_tilt).reshape(slot_total).astype(jnp.int32)
    view_index = slot_view.reshape(slot_total).astype(jnp.int32)
    weights = node_weights(slot_pos[0].reshape(slot_total).astype(jnp.float32), slot_pos[1].reshape(slot_total).astype(jnp.float32), GRID)
    shifts = lax.optimization_barrier(jnp.sum(warp_grid[tilt_index] * weights[:, None, :], axis=2))
    focus = defocus.reshape(slot_total).astype(jnp.float32)
    freq_rows = jnp.arange(PATCH, dtype=jnp.int32)
    row_table, col_table = dft_tables(freq_rows, PATCH)
    block_len = math.gcd(slot_total, 32)
    block_count = slot_total // block_len

    def one_block(inputs):
        patch_blk, view_blk, tilt_blk, focus_blk, shift_blk = inputs
        ref_blk = projections[view_blk, tilt_blk]
        first_pass = jnp.einsum('fy,byx->bfx', row_table.astype(jnp.float32), patch_blk.astype(jnp.float32)).astype(jnp.bfloat16)
        spectrum = jnp.einsum('bfx,xk->bfk', first_pass.astype(jnp.float32), col_table.astype(jnp.float32))
        return spectral_terms(spectrum, ref_blk, focus_blk, shift_blk, freq_rows, PATCH)
    per_slot = lax.map(one_block, (patches.reshape(block_count, block_len, PATCH, PATCH), view_index.reshape(block_count, block_len), tilt_index.reshape(block_count, block_len), focus.reshape(block_count, block_len), shifts.reshape(block_count, block_len, 2))).reshape(slot_total, 3)
    slot_terms = per_slot.T.reshape(3, N_TILT, SLOTS)
    tilt_hits = (tilt_index[:, None] == jnp.arange(TILTS, dtype=jnp.int32)[None, :]).astype(jnp.float32)
    node_coef = (tilt_hits[:, :, None] * per_slot[:, None, 1:3]).reshape(slot_total, 2 * TILTS)
    gradient = jnp.dot(node_coef.T, weights, precision=lax.Precision.HIGHEST, preferred_element_type=jnp.float32).reshape(TILTS, 2, NODES)
    new_warp = warp_grid - gradient / jnp.sqrt(gradient * gradient + TRUST_FLOOR * TRUST_FLOOR)
    return (slot_terms, new_warp)
```

```python
import functools
import math

import jax
import jax.numpy as jnp
from jax import lax
from jax.experimental import pallas as pl
from jax.experimental.pallas import tpu as pltpu
from jax.sharding import PartitionSpec as P

GRID = 16
AMPLITUDE = 0.07
TRUST_FLOOR = 0.02


def signed_freq(index, pixels):
    return jnp.where(index < pixels // 2, index, index - pixels).astype(jnp.float32)


def dft_tables(freq_rows, pixels):
    columns = jnp.arange(pixels, dtype=jnp.int32)
    table_scale = 1.0 / math.sqrt(pixels)
    turns_rows = (freq_rows[:, None] * columns[None, :] % pixels).astype(jnp.float32) * (
        2.0 * math.pi / pixels
    )
    turns_full = (columns[:, None] * columns[None, :] % pixels).astype(jnp.float32) * (
        2.0 * math.pi / pixels
    )
    row_table = jnp.concatenate([jnp.cos(turns_rows), jnp.sin(turns_rows)], axis=0) * table_scale
    col_table = jnp.concatenate([jnp.cos(turns_full), jnp.sin(turns_full)], axis=1) * table_scale
    return (row_table.astype(jnp.bfloat16), col_table.astype(jnp.bfloat16))


def node_weights(pos_x, pos_y, grid_side):
    knot_pos = jnp.arange(grid_side, dtype=jnp.int32).astype(jnp.float32)
    weight_x = jnp.maximum(0.0, 1.0 - jnp.abs(pos_x[:, None] * (grid_side - 1) - knot_pos[None, :]))
    weight_y = jnp.maximum(0.0, 1.0 - jnp.abs(pos_y[:, None] * (grid_side - 1) - knot_pos[None, :]))
    return (weight_y[:, :, None] * weight_x[:, None, :]).reshape(
        pos_x.shape[0], grid_side * grid_side
    )


def contrast_of(focus, radius):
    aberration = math.pi * focus * radius
    return -(
        math.sqrt(1.0 - AMPLITUDE * AMPLITUDE) * jnp.sin(aberration)
        + AMPLITUDE * jnp.cos(aberration)
    )


def fold_kernel(rep_ref, own_ref, recv_ref, fold_ref, spread_ref):
    first = rep_ref[0] == 0
    pairs, half, pixels = own_ref.shape[1], recv_ref.shape[3], own_ref.shape[4]
    rows = 2 * half
    col_a = lax.broadcasted_iota(jnp.int32, (pixels, pixels), 0)
    col_b = lax.broadcasted_iota(jnp.int32, (pixels, pixels), 1)
    flip_cols = ((col_a + col_b) % pixels == 0).astype(jnp.bfloat16)
    row_a = lax.broadcasted_iota(jnp.int32, (rows, 2 * rows), 0)
    row_b = lax.broadcasted_iota(jnp.int32, (rows, 2 * rows), 1)
    flip_rows = (
        (row_a // half == row_b // rows) & (row_a % half + row_b % rows == half)
    ).astype(jnp.bfloat16)
    lane = lax.broadcasted_iota(jnp.int32, (half, pixels), 1)
    line = lax.broadcasted_iota(jnp.int32, (half, pixels), 0)
    whole = jnp.logical_and(line == 0, first)
    alone = jnp.logical_or(whole, lane == pixels // 2)
    for p in range(pairs):
        near, far = [], []
        for c in range(2):
            own = own_ref[0, p, c]
            recv = recv_ref[0, p, c]
            near.append(jnp.where(first, own[:half], recv).astype(jnp.float32))
            far.append(jnp.where(first, recv, own[:half]))
            far.append(own[half:])
        mirror = jnp.dot(
            jnp.concatenate(far, axis=0), flip_cols, preferred_element_type=jnp.float32
        ).astype(jnp.bfloat16)
        mirror = jnp.dot(flip_rows, mirror, preferred_element_type=jnp.float32)
        mir_re, mir_im = mirror[:half], mirror[half:]
        even_re = jnp.where(whole, near[0], 0.5 * (near[0] + mir_re))
        even_im = jnp.where(whole, near[1], 0.5 * (near[1] - mir_im))
        odd_re = 0.5 * (near[0] - mir_re)
        odd_im = 0.5 * (near[1] + mir_im)
        base = p * rows
        fold_ref[base : base + half, :] = even_re.astype(jnp.bfloat16)
        fold_ref[base + half : base + rows, :] = even_im.astype(jnp.bfloat16)
        spread_ref[p] = jnp.where(alone, 0.0, 2.0 * (odd_re * odd_re + odd_im * odd_im))


def folded(own, recv, rep_index, total_rows):
    views, tilts, _, rows, pixels = own.shape
    half = rows // 2
    return pl.pallas_call(
        fold_kernel,
        grid=(views,),
        in_specs=[
            pl.BlockSpec(memory_space=pltpu.SMEM),
            pl.BlockSpec((1, tilts, 2, rows, pixels), lambda v: (v, 0, 0, 0, 0)),
            pl.BlockSpec((1, tilts, 2, half, pixels), lambda v: (v, 0, 0, 0, 0)),
        ],
        out_specs=[
            pl.BlockSpec((tilts * rows, pixels), lambda v: (v, 0)),
            pl.BlockSpec((tilts, half, pixels), lambda v: (v, 0, 0)),
        ],
        out_shape=[
            jax.ShapeDtypeStruct((total_rows, pixels), jnp.bfloat16),
            jax.ShapeDtypeStruct((views * tilts, half, pixels), jnp.float32),
        ],
        name="fold",
    )(rep_index, own, recv)


def on_device(patches, slot_view, slot_tilt, slot_pos, defocus, projections, warp_grid):
    owners = lax.axis_size("dom")
    rep = lax.axis_index("rep")
    slot_count = patches.shape[1]
    pixels = patches.shape[-1]
    view_dev = projections.shape[0]
    tilt_dev = warp_grid.shape[0]
    node_count = warp_grid.shape[2]
    pair_dev = view_dev * tilt_dev
    rows = projections.shape[3]
    half = rows // 2
    nyquist = pixels // 2
    capacity = 3 * slot_count // (2 * owners)
    buffer_len = owners * capacity
    first = rep == 0

    swap = [(i, 1 - i) for i in range(2)]
    recv = lax.ppermute(projections[:, :, :, half:], "rep", swap)
    main_rows = pair_dev * rows
    block_rows = -(-(3 * pair_dev) // rows) * rows
    total_rows = main_rows + block_rows
    payload, spread = folded(projections, recv, jnp.reshape(rep, (1,)).astype(jnp.int32), total_rows)
    own_col = projections[..., nyquist]
    recv_col = recv[..., nyquist]
    near_col = jnp.where(first, own_col[..., :half], recv_col)
    far_col = jnp.where(
        first,
        jnp.concatenate([recv_col, own_col[..., half:]], axis=-1)[..., 1 : half + 1],
        own_col[..., 1 : half + 1],
    )
    far_col = jnp.flip(far_col, axis=-1)
    edge_line = jnp.concatenate([projections[:, :, :, 0], near_col, far_col], axis=-1)
    payload = lax.dynamic_update_slice(payload, edge_line.reshape(3 * pair_dev, pixels), (main_rows, 0))
    gathered = lax.all_gather(payload, "dom", axis=0, tiled=True)

    chosen_view = slot_view[0, :, 0]
    tilt_local = slot_tilt[0]
    owner_of = chosen_view // view_dev
    pair_of = (chosen_view % view_dev) * tilt_dev + tilt_local
    focus = defocus[0].astype(jnp.float32)
    owner_hits = (owner_of[:, None] == jnp.arange(owners, dtype=jnp.int32)[None, :]).astype(
        jnp.int32
    )
    earlier = jnp.cumsum(owner_hits, axis=0) - owner_hits
    slot_rank = jnp.sum(earlier * owner_hits, axis=1)
    target = owner_of * capacity + slot_rank
    matches = target[None, :] == jnp.arange(buffer_len, dtype=jnp.int32)[:, None]
    asked = jnp.stack(
        [
            jnp.sum(jnp.where(matches, pair_of[None, :].astype(jnp.float32), 0.0), axis=1),
            jnp.sum(jnp.where(matches, focus[None, :], 0.0), axis=1),
        ],
        axis=1,
    ).reshape(owners, capacity * 2)

    main_y = signed_freq(rep * half + jnp.arange(half, dtype=jnp.int32), pixels)
    freq_x = signed_freq(jnp.arange(pixels, dtype=jnp.int32), pixels)
    scale_q = 1.0 / (nyquist * nyquist)
    main_q = (main_y[:, None] * main_y[:, None] + freq_x[None, :] * freq_x[None, :]) * scale_q
    heard = lax.all_to_all(asked, "dom", 0, 0, tiled=True).reshape(buffer_len, 2)
    heard_pair = heard[:, 0].astype(jnp.int32)
    heard_ctf = contrast_of(heard[:, 1, None, None], main_q[None])
    apart = jnp.sum(heard_ctf * heard_ctf * spread[heard_pair], axis=(1, 2))
    answer = lax.all_to_all(apart.reshape(owners, capacity), "dom", 0, 0, tiled=True)
    apart_slot = jnp.sum(jnp.where(matches, answer.reshape(buffer_len)[:, None], 0.0), axis=0)

    weights = node_weights(
        slot_pos[0, 0].astype(jnp.float32), slot_pos[1, 0].astype(jnp.float32), GRID
    )
    tilt_match = tilt_local[:, None] == jnp.arange(tilt_dev, dtype=jnp.int32)[None, :]
    shifts = jnp.sum(warp_grid[tilt_local] * weights[:, None, :], axis=2)
    row_table, col_table = dft_tables(
        jnp.concatenate(
            [rep * half + jnp.arange(half, dtype=jnp.int32), jnp.full((1,), nyquist, jnp.int32)]
        ),
        pixels,
    )
    main_table = jnp.concatenate([row_table[:half], row_table[half + 1 : 2 * half + 1]], axis=0)
    edge_table = jnp.concatenate([row_table[half : half + 1], row_table[2 * half + 1 :]], axis=0)

    def spectrum_of(table, count):
        first_pass = jnp.einsum(
            "fy,byx->bfx", table, patches[0], preferred_element_type=jnp.float32
        ).astype(jnp.bfloat16)
        both = jnp.einsum("bfx,xk->bfk", first_pass, col_table, preferred_element_type=jnp.float32)
        real = both[:, :count, :pixels] - both[:, count:, pixels:]
        imag = -(both[:, :count, pixels:] + both[:, count:, :pixels])
        return real, imag

    main_re, main_im = spectrum_of(main_table, half)
    edge_re, edge_im = spectrum_of(edge_table, 1)
    turn = 2.0 * math.pi / pixels
    main_phase = turn * (
        freq_x[None, None, :] * shifts[:, 0, None, None]
        + main_y[None, :, None] * shifts[:, 1, None, None]
    )
    main_cos, main_sin = jnp.cos(main_phase), jnp.sin(main_phase)
    turned_re = main_re * main_cos - main_im * main_sin
    turned_im = main_re * main_sin + main_im * main_cos
    main_ctf = contrast_of(focus[:, None, None], main_q[None])
    col_re, col_im = main_re[:, :, nyquist], main_im[:, :, nyquist]
    line_re = jnp.concatenate([edge_re[:, 0], col_re, col_re], axis=1)
    line_im = jnp.concatenate([edge_im[:, 0], col_im, -col_im], axis=1)
    line_x = jnp.concatenate([freq_x, jnp.full((2 * half,), -float(nyquist), jnp.float32)])
    line_y = jnp.concatenate([jnp.full((pixels,), -float(nyquist), jnp.float32), main_y, -main_y])
    line_weight = jnp.concatenate(
        [
            jnp.full((pixels,), jnp.where(first, 0.0, 1.0)),
            jnp.where(main_y == 0.0, 0.0, 1.0),
            jnp.where(main_y == 0.0, 0.0, 1.0),
        ]
    )
    line_q = (line_x * line_x + line_y * line_y) * scale_q
    line_phase = turn * (line_x[None] * shifts[:, 0, None] + line_y[None] * shifts[:, 1, None])
    line_cos, line_sin = jnp.cos(line_phase), jnp.sin(line_phase)
    line_ctf = contrast_of(focus[:, None], line_q[None])
    turned_line_re = line_re * line_cos - line_im * line_sin
    turned_line_im = line_re * line_sin + line_im * line_cos
    main_weight = jnp.where(
        main_y[:, None] == 0.0, 1.0, jnp.where(freq_x[None, :] == -float(nyquist), 0.0, 2.0)
    )
    held = lax.optimization_barrier(
        (
            turned_re,
            turned_im,
            main_ctf,
            turned_line_re,
            turned_line_im,
            line_ctf,
            apart_slot,
            weights,
            main_weight,
        )
    )
    (turned_re, turned_im, main_ctf, turned_line_re, turned_line_im, line_ctf) = held[:6]
    apart_slot, weights, main_weight = held[6:]

    per_owner = total_rows // rows
    ref_blk = gathered.reshape(owners * per_owner, rows, pixels)[owner_of * per_owner + pair_of]
    line_at = (owner_of * total_rows + main_rows + 3 * pair_of)[:, None] + jnp.arange(3)[None]
    line_blk = gathered[line_at.reshape(-1)].reshape(slot_count, 3 * pixels)

    def terms(spin_re, spin_im, ctf, ref_re, ref_im, weight, fx, fy, axes):
        model_re = ctf * ref_re.astype(jnp.float32)
        model_im = ctf * ref_im.astype(jnp.float32)
        diff_re = spin_re - model_re
        diff_im = spin_im - model_im
        cross = weight * (diff_im * model_re - diff_re * model_im)
        return (
            jnp.sum(weight * (diff_re * diff_re + diff_im * diff_im), axis=axes),
            jnp.sum(turn * fx * cross, axis=axes),
            jnp.sum(turn * fy * cross, axis=axes),
        )

    main_terms = terms(
        turned_re,
        turned_im,
        main_ctf,
        ref_blk[:, :half],
        ref_blk[:, half:],
        main_weight[None],
        freq_x[None, None, :],
        main_y[None, :, None],
        (1, 2),
    )
    line_len = 3 * pixels // 2
    line_terms = terms(
        turned_line_re,
        turned_line_im,
        line_ctf,
        line_blk[:, :line_len],
        line_blk[:, line_len:],
        line_weight[None],
        line_x[None],
        line_y[None],
        1,
    )
    inverse_area = 1.0 / (pixels * pixels)
    energy = (main_terms[0] + line_terms[0] + apart_slot) * inverse_area
    grad_x = 2.0 * inverse_area * (main_terms[1] + line_terms[1])
    grad_y = 2.0 * inverse_area * (main_terms[2] + line_terms[2])
    per_slot = jnp.stack([energy, grad_x, grad_y], axis=0)

    spot = tilt_match.astype(jnp.float32).T[:, None, :]
    node_coef = (spot * per_slot[None, 1:3]).reshape(2 * tilt_dev, slot_count)
    gradient = jnp.dot(
        node_coef, weights, precision=lax.Precision.HIGHEST, preferred_element_type=jnp.float32
    )
    per_slot, gradient = lax.psum((per_slot, gradient), "rep")
    slot_terms = per_slot[:, None, :]
    node_share = node_count // owners
    tiles = gradient.reshape(2 * tilt_dev, owners, node_share).transpose(1, 0, 2)
    tiles = lax.all_to_all(tiles.reshape(owners, -1), "dom", 0, 0, tiled=True)
    share_grad = jnp.sum(tiles, axis=0).reshape(tilt_dev, 2, node_share)
    warp_share = lax.dynamic_slice_in_dim(
        warp_grid, lax.axis_index("dom") * node_share, node_share, 2
    )
    moved = warp_share - share_grad / jnp.sqrt(share_grad * share_grad + TRUST_FLOOR * TRUST_FLOOR)
    spread_out = lax.all_to_all(
        jnp.broadcast_to(moved.reshape(1, -1), (owners, moved.size)), "dom", 0, 0, tiled=True
    )
    new_warp = (
        spread_out.reshape(owners, tilt_dev, 2, node_share)
        .transpose(1, 2, 0, 3)
        .reshape(tilt_dev, 2, node_count)
    )
    return (slot_terms, new_warp)


def solution(mesh):
    in_specs = (
        P(("groups", "tilt"), "dom", None, None),
        P(("groups", "tilt"), "dom", None),
        P(("groups", "tilt"), "dom"),
        P(None, ("groups", "tilt"), "dom"),
        P(("groups", "tilt"), "dom"),
        P(("groups", "dom"), "tilt", None, "rep", None),
        P(("groups", "tilt"), None, None),
    )
    out_specs = (P(None, ("groups", "tilt"), "dom"), P(("groups", "tilt"), None, None))
    return jax.shard_map(
        on_device, mesh=mesh, in_specs=in_specs, out_specs=out_specs, check_vma=False
    )
```

```python
import functools
import math

import jax
import jax.numpy as jnp
import numpy as np
from jax import lax
from jax.experimental import pallas as pl
from jax.experimental.pallas import tpu as pltpu
from jax.sharding import PartitionSpec as P


GRID = 16
AMPLITUDE = 0.07
TRUST_FLOOR = 0.02
RADIUS = 8
CHUNKS = 2
GROUP = 8
EXTRA = 4
BIG = math.sqrt(1.0 - AMPLITUDE * AMPLITUDE)


def signed_freq(pixels):
    index = np.arange(pixels)
    return np.where(index < pixels // 2, index, index - pixels).astype(np.float32)


def dft_tables(pixels):
    index = np.arange(pixels)
    angle = (index[:, None] * index[None, :] % pixels) * (2.0 * math.pi / pixels)
    scale = 1.0 / math.sqrt(pixels)
    return tuple(
        np.asarray(t * scale, np.float32).astype(jnp.bfloat16) for t in (np.cos(angle), np.sin(angle))
    )


def node_weights(pos_x, pos_y, grid_side):
    knot_pos = jnp.arange(grid_side, dtype=jnp.int32).astype(jnp.float32)
    weight_x = jnp.maximum(0.0, 1.0 - jnp.abs(pos_x[:, None] * (grid_side - 1) - knot_pos[None, :]))
    weight_y = jnp.maximum(0.0, 1.0 - jnp.abs(pos_y[:, None] * (grid_side - 1) - knot_pos[None, :]))
    return (weight_y[:, :, None] * weight_x[:, None, :]).reshape(
        pos_x.shape[0], grid_side * grid_side
    )


def iota(shape, dim):
    return lax.broadcasted_iota(jnp.int32, shape, dim)


def line_dot(a, b):
    return lax.dot_general(a, b, (((1,), (1,)), ((), ())), preferred_element_type=jnp.float32)


def fold_kernel(rep_ref, own_ref, recv_ref, out_ref, spread_ref):
    first = rep_ref[0] == 0
    views, tilts, half, pixels = own_ref.shape[0], own_ref.shape[1], own_ref.shape[3], own_ref.shape[4]
    flip_cols = ((iota((pixels, pixels), 0) + iota((pixels, pixels), 1)) % pixels == 0).astype(
        jnp.bfloat16
    )
    row_a, row_b = iota((2 * half, 2 * half), 0), iota((2 * half, 2 * half), 1)
    flip_rows = (
        (row_a // half == row_b // half) & (row_a % half + row_b % half == half)
    ).astype(jnp.bfloat16)
    at_edge = (iota((16, pixels), 1) == pixels // 2).astype(jnp.bfloat16)
    lane, line = iota((half, pixels), 1), iota((half, pixels), 0)
    whole = line == 0
    alone = jnp.logical_or(whole, lane == pixels // 2)
    count = views * tilts
    extras = []
    batch = 5
    for start in range(0, count, batch):
        lows, boths = [], []
        for p in range(start, start + batch):
            v, t = p // tilts, p % tilts
            own, recv = own_ref[v, t], recv_ref[v, t]
            lows.append(jnp.where(first, own, recv).reshape(2 * half, pixels))
            boths.append(jnp.where(first, recv, own).reshape(2 * half, pixels))
        turned = jnp.dot(
            jnp.concatenate(boths, axis=0), flip_cols, preferred_element_type=jnp.float32
        ).astype(jnp.bfloat16)
        mirrors = [
            jnp.dot(
                flip_rows,
                turned[2 * half * i : 2 * half * (i + 1)],
                preferred_element_type=jnp.float32,
            )
            for i in range(batch)
        ]
        cols = [
            line_dot(at_edge, jnp.concatenate([low, mirror.astype(jnp.bfloat16)], axis=0))
            for low, mirror in zip(lows, mirrors, strict=True)
        ]
        for i in range(batch):
            p = start + i
            low, mirror = lows[i].astype(jnp.float32), mirrors[i]
            low_re, low_im, mir_re, mir_im = low[:half], low[half:], mirror[:half], mirror[half:]
            base = p * 2 * half
            even_re = jnp.where(whole, low_re, 0.5 * (low_re + mir_re))
            even_im = jnp.where(whole, low_im, 0.5 * (low_im - mir_im))
            out_ref[base : base + half, :] = even_re.astype(jnp.bfloat16)
            out_ref[base + half : base + 2 * half, :] = even_im.astype(jnp.bfloat16)
            odd_re, odd_im = 0.5 * (low_re - mir_re), 0.5 * (low_im + mir_im)
            spread_ref[p] = jnp.where(alone, 0.0, 2.0 * (odd_re * odd_re + odd_im * odd_im))
            both = boths[i].astype(jnp.float32)
            col = cols[i][0:1]
            extras += [
                both[0:1],
                both[half : half + 1],
                jnp.concatenate([col[:, :half], col[:, 2 * half : 3 * half]], axis=1),
                jnp.concatenate([col[:, half : 2 * half], col[:, 3 * half :]], axis=1),
            ]
    top = count * 2 * half
    for g in range(count * EXTRA // 16):
        out_ref[top + 16 * g : top + 16 * (g + 1), :] = jnp.concatenate(
            extras[16 * g : 16 * (g + 1)], axis=0
        ).astype(jnp.bfloat16)


def folded(own, recv, rep_index, chunk):
    views, tilts, _, half, pixels = own.shape
    per = views // CHUNKS
    count = per * tilts
    rows = count * (2 * half + EXTRA)
    return pl.pallas_call(
        fold_kernel,
        grid=(1,),
        in_specs=[
            pl.BlockSpec(memory_space=pltpu.SMEM),
            pl.BlockSpec((per, tilts, 2, half, pixels), lambda v: (chunk, 0, 0, 0, 0)),
            pl.BlockSpec((per, tilts, 2, half, pixels), lambda v: (chunk, 0, 0, 0, 0)),
        ],
        out_specs=[
            pl.BlockSpec((rows, pixels), lambda v: (0, 0)),
            pl.BlockSpec((count, half, pixels), lambda v: (0, 0, 0)),
        ],
        out_shape=[
            jax.ShapeDtypeStruct((rows, pixels), jnp.bfloat16),
            jax.ShapeDtypeStruct((count, half, pixels), jnp.float32),
        ],
        name="fold",
    )(rep_index, own, recv)


def dft_kernel(src_ref, patch_ref, row_ref, col_ref, side_ref, rt_ref, ct_ref, *outs, start):
    out_re, out_im, out_ctf, edge_ref = outs
    step = pl.program_id(0) + start
    pixels = col_ref.shape[0]
    half = pixels // 2
    rt = rt_ref[0]
    for k in range(GROUP):
        patch = patch_ref[src_ref[step * GROUP + k]]
        first = jnp.dot(row_ref[...], patch, preferred_element_type=jnp.float32).astype(jnp.bfloat16)
        both = jnp.dot(first, col_ref[...], preferred_element_type=jnp.float32)
        re = both[:half, :pixels] - both[half:pixels, pixels:]
        im = -(both[:half, pixels:] + both[half:pixels, :pixels])
        cy, sy = rt[:, k : k + 1], rt[:, GROUP + k : GROUP + k + 1]
        qc = rt[:, 2 * GROUP + k : 2 * GROUP + k + 1]
        qs = rt[:, 3 * GROUP + k : 3 * GROUP + k + 1]
        cx, sx, pc, ps = (ct_ref[i, k : k + 1, :] for i in range(4))
        er = cy * cx - sy * sx
        ei = sy * cx + cy * sx
        out_re[k] = re * er - im * ei
        out_im[k] = re * ei + im * er
        out_ctf[k] = qc * pc + qs * ps
        side = line_dot(side_ref[...], first[:pixels])
        low, high = both[pixels : pixels + 1], both[pixels + 1 : pixels + 2]
        edge_ref[0, k : k + 1, :] = low[:, :pixels] - high[:, pixels:]
        edge_ref[1, k : k + 1, :] = -(low[:, pixels:] + high[:, :pixels])
        edge_ref[2, k : k + 1, :] = side[0:1]
        edge_ref[3, k : k + 1, :] = side[1:2]


def spectra(src, patches, row_table, col_table, side_table, row_tab, col_tab, start, groups):
    _, half, pixels = row_tab.shape
    slots = groups * GROUP
    tall = row_table.shape[0]
    plane = pl.BlockSpec((GROUP, half, pixels), lambda g: (g, 0, 0))
    shape = jax.ShapeDtypeStruct((slots, half, pixels), jnp.float32)
    return pl.pallas_call(
        functools.partial(dft_kernel, start=start),
        grid=(groups,),
        in_specs=[
            pl.BlockSpec(memory_space=pltpu.SMEM),
            pl.BlockSpec(patches.shape, lambda g: (0, 0, 0)),
            pl.BlockSpec((tall, pixels), lambda g: (0, 0)),
            pl.BlockSpec((pixels, 2 * pixels), lambda g: (0, 0)),
            pl.BlockSpec(side_table.shape, lambda g: (0, 0)),
            pl.BlockSpec((1, half, pixels), lambda g: (g + start, 0, 0)),
            pl.BlockSpec((4, GROUP, pixels), lambda g: (0, g + start, 0)),
        ],
        out_specs=[plane, plane, plane, pl.BlockSpec((4, GROUP, pixels), lambda g: (0, g, 0))],
        out_shape=[shape, shape, shape, jax.ShapeDtypeStruct((4, slots, pixels), jnp.float32)],
        cost_estimate=pl.CostEstimate(flops=10**9 * groups, bytes_accessed=2 * 10**7, transcendentals=0),
        name="spectra",
    )(src, patches, row_table, col_table, side_table, row_tab, col_tab)


def chosen(refs, pair, start, size, stride):
    per = refs[0][1]
    rows = None
    for i, (ref, count) in enumerate(refs):
        q = jnp.clip(pair - i * per, 0, count - 1)
        at = pl.multiple_of(start(count, q), stride)
        part = ref[pl.ds(at, size), :]
        rows = part if rows is None else jnp.where(pair >= i * per, part, rows)
    return rows


def extra_rows(refs, pair, pixels):
    return chosen(refs, pair, lambda n, q: n * pixels + (q // 4) * 16, 16, 16)


def terms_kernel(ids_ref, *refs, sources, base, cap):
    at, held_by = 0, []
    for counts, _ in sources:
        held_by.append(list(zip(refs[at : at + len(counts)], counts, strict=True)))
        at += len(counts)
    re_ref, im_ref, ctf_ref, line_ref, out_ref = refs[at:]
    _, half, pixels = re_ref.shape
    line, lane = iota((half, pixels), 0), iota((half, pixels), 1)
    weight = jnp.where(line == 0, 1.0, jnp.where(lane == half, 0.0, 2.0))
    fy = line.astype(jnp.float32)
    edge = iota((1, pixels), 1)
    col_weight = jnp.where(edge % half == 0, 0.0, 1.0)
    col_fy = jnp.where(edge < half, edge, half - edge).astype(jnp.float32)
    for n, (counts, fixed) in enumerate(sources):
        held = held_by[n]
        for k in range(cap):
            i = n * cap + k
            pair = jnp.int32(k) if fixed else ids_ref[base + i]
            ref_blk = chosen(held, pair, lambda m, q: q * pixels, pixels, pixels).astype(jnp.float32)
            group = extra_rows(held, pair, pixels)
            picker = iota((8, 16), 1) == 4 * ((pair % counts[0]) % 4) + iota((8, 16), 0)
            rim = jnp.dot(picker.astype(jnp.bfloat16), group, preferred_element_type=jnp.float32)
            ctf = ctf_ref[i]
            mod_re, mod_im = ctf * ref_blk[:half], ctf * ref_blk[half:]
            dif_re, dif_im = re_ref[i] - mod_re, im_ref[i] - mod_im
            power = weight * (dif_re * dif_re + dif_im * dif_im)
            cross = weight * (dif_im * mod_re - dif_re * mod_im)
            own = [line_ref[j, i : i + 1, :] for j in range(6)]

            def edge_terms(a, b, own=own, rim=rim):
                m_re, m_im = own[a + 2] * rim[b : b + 1], own[a + 2] * rim[b + 1 : b + 2]
                d_re, d_im = own[a] - m_re, own[a + 1] - m_im
                return d_re * d_re + d_im * d_im, d_im * m_re - d_re * m_im

            row_power, row_cross = edge_terms(0, 0)
            col_power, col_cross = edge_terms(3, 2)
            col_cross = col_weight * col_cross
            out_ref[0, i : i + 1, :] = (
                jnp.sum(power, axis=0, keepdims=True) + row_power + col_weight * col_power
            )
            out_ref[1, i : i + 1, :] = jnp.sum(cross, axis=0, keepdims=True) + row_cross
            out_ref[2, i : i + 1, :] = (
                jnp.sum(fy * cross, axis=0, keepdims=True) - half * row_cross + col_fy * col_cross
            )
            out_ref[3, i : i + 1, :] = col_cross


def terms_of(first_hop, ids, sources, turned, cap):
    re, im, ctf, line = turned
    _, half, pixels = re.shape
    number = len(sources) * cap
    arrays = [a for blocks, _, _ in sources for a in blocks]
    plane = pl.BlockSpec((number, half, pixels), lambda g: (0, 0, 0))
    return pl.pallas_call(
        functools.partial(
            terms_kernel, sources=[(c, f) for _, c, f in sources], base=first_hop * cap, cap=cap
        ),
        grid=(1,),
        in_specs=[pl.BlockSpec(memory_space=pltpu.SMEM)]
        + [pl.BlockSpec(a.shape, lambda g: (0, 0)) for a in arrays]
        + [plane, plane, plane, pl.BlockSpec(line.shape, lambda g: (0, 0, 0))],
        out_specs=pl.BlockSpec((4, number, pixels), lambda g: (0, 0, 0)),
        out_shape=jax.ShapeDtypeStruct((4, number, pixels), jnp.float32),
        cost_estimate=pl.CostEstimate(flops=10**9, bytes_accessed=10**7, transcendentals=0),
        name="terms",
    )(ids, *arrays, re, im, ctf, line)


def pick_kernel(ids_ref, *refs, counts, cap, caps):
    held = list(zip(refs[: len(counts)], counts, strict=True))
    pixels = refs[0].shape[1]
    for j, out in enumerate(refs[len(counts) :]):
        groups = [None] * (-(-caps[j] * EXTRA // 16))
        for k in range(caps[j]):
            pair = ids_ref[j * cap + k]
            out[k * pixels : (k + 1) * pixels, :] = chosen(
                held, pair, lambda n, q: q * pixels, pixels, pixels
            )
            group = extra_rows(held, pair, pixels)
            row, col = iota((16, 16), 0), iota((16, 16), 1)
            mover = (row // 4 == k % 4) & (col // 4 == (pair % counts[0]) % 4) & (row % 4 == col % 4)
            moved = jnp.dot(mover.astype(jnp.bfloat16), group, preferred_element_type=jnp.float32)
            g = k // 4
            groups[g] = moved if groups[g] is None else groups[g] + moved
        for g, rows in enumerate(groups):
            at = caps[j] * pixels + 16 * g
            out[at : at + 16, :] = rows.astype(jnp.bfloat16)


def picked(ids, blocks, counts, cap, caps):
    pixels = blocks[0].shape[1]
    rows = [c * pixels + 16 * (-(-c * EXTRA // 16)) for c in caps]
    return pl.pallas_call(
        functools.partial(pick_kernel, counts=counts, cap=cap, caps=caps),
        grid=(1,),
        in_specs=[pl.BlockSpec(memory_space=pltpu.SMEM)]
        + [pl.BlockSpec(b.shape, lambda g: (0, 0)) for b in blocks],
        out_specs=[pl.BlockSpec((r, pixels), lambda g: (0, 0)) for r in rows],
        out_shape=[jax.ShapeDtypeStruct((r, pixels), jnp.bfloat16) for r in rows],
        name="pick",
    )(ids, *blocks)


def apart_kernel(ids_ref, *refs, counts):
    held = refs[: len(counts)]
    rt_ref, ct_ref, out_ref = refs[len(counts) :]
    step = pl.program_id(0)
    rt = rt_ref[0]
    for k in range(GROUP):
        pair = ids_ref[step * GROUP + k]
        power = None
        for i, (ref, count) in enumerate(zip(held, counts, strict=True)):
            part = ref[jnp.clip(pair - i * counts[0], 0, count - 1)]
            power = part if power is None else jnp.where(pair >= i * counts[0], part, power)
        ctf = (
            rt[:, k : k + 1] * ct_ref[0, k : k + 1, :]
            + rt[:, GROUP + k : GROUP + k + 1] * ct_ref[1, k : k + 1, :]
        )
        out_ref[k : k + 1, :] = jnp.sum(ctf * ctf * power, axis=0, keepdims=True)


def apart_of(ids, spreads, counts, row_tab, col_tab):
    groups, half, pixels = row_tab.shape
    return pl.pallas_call(
        functools.partial(apart_kernel, counts=counts),
        grid=(groups,),
        in_specs=[pl.BlockSpec(memory_space=pltpu.SMEM)]
        + [pl.BlockSpec(s.shape, lambda g: (0, 0, 0)) for s in spreads]
        + [
            pl.BlockSpec((1, half, pixels), lambda g: (g, 0, 0)),
            pl.BlockSpec((2, GROUP, pixels), lambda g: (0, g, 0)),
        ],
        out_specs=pl.BlockSpec((GROUP, pixels), lambda g: (g, 0)),
        out_shape=jax.ShapeDtypeStruct((groups * GROUP, pixels), jnp.float32),
        cost_estimate=pl.CostEstimate(flops=10**9, bytes_accessed=4 * 10**6, transcendentals=0),
        name="apart",
    )(ids, *spreads, row_tab, col_tab)


def lane_tables(tables, pixels):
    stacked = jnp.stack(tables, axis=0)
    count, slots, rows = stacked.shape
    laid = stacked.reshape(count, slots // GROUP, GROUP, rows).transpose(1, 3, 0, 2)
    laid = laid.reshape(slots // GROUP, rows, count * GROUP)
    return jnp.pad(laid, ((0, 0), (0, 0), (0, pixels - count * GROUP)))


def contrast_tables(focus, low_y, freq_x, nyquist):
    rate = math.pi * focus[:, None] / (nyquist * nyquist)
    by, bx = rate * (low_y * low_y)[None], rate * (freq_x * freq_x)[None]
    sin_x, cos_x = jnp.sin(bx), jnp.cos(bx)
    pc = -(BIG * sin_x + AMPLITUDE * cos_x)
    ps = -(BIG * cos_x - AMPLITUDE * sin_x)
    return jnp.cos(by), jnp.sin(by), pc, ps


def contrast_of(focus, radius):
    aberration = math.pi * focus * radius
    return -(BIG * jnp.sin(aberration) + AMPLITUDE * jnp.cos(aberration))


def on_device(patches, slot_view, slot_tilt, slot_pos, defocus, projections, warp_grid):
    owners = lax.axis_size("dom")
    me = lax.axis_index("dom")
    rep = lax.axis_index("rep")
    first = rep == 0
    slot_count = patches.shape[1]
    pixels = patches.shape[-1]
    half = nyquist = pixels // 2
    view_dev = projections.shape[0]
    tilt_dev = warp_grid.shape[0]
    node_count = warp_grid.shape[2]
    pair_dev = view_dev * tilt_dev
    cap = 3 * slot_count // (2 * owners)
    reach = owners // 2
    hops = reach + 1
    used = hops * cap
    slots = -(-used // GROUP) * GROUP
    counts = (pair_dev // CHUNKS,) * CHUNKS
    turn = 2.0 * math.pi / pixels
    scale_q = 1.0 / (nyquist * nyquist)

    recv = lax.ppermute(projections, "rep", [(0, 1), (1, 0)])
    rep_index = jnp.reshape(rep, (1,)).astype(jnp.int32)
    made = []
    for c in range(CHUNKS):
        made.append(folded(projections, recv, rep_index, c))
    blocks = [m[0] for m in made]
    spreads = [m[1] for m in made]

    def ring(shift):
        pairs = []
        for i in range(owners):
            pairs.append((2 * i, 2 * ((i + shift) % owners)))
            pairs.append((2 * i + 1, 2 * ((i - shift) % owners) + 1))
        return pairs

    ring_blocks = [blocks]
    for _ in range(1, RADIUS + 1):
        sent = []
        for block in ring_blocks[-1]:
            sent.append(lax.ppermute(block, ("dom", "rep"), ring(1)))
        ring_blocks.append(sent)

    later = made[0][1][0, 0, 0].astype(jnp.int32)

    chosen_view = slot_view[0, :, 0]
    owner_of = chosen_view // view_dev
    pair_of = (chosen_view % view_dev) * tilt_dev + slot_tilt[0]
    hits = (owner_of[:, None] == jnp.arange(owners, dtype=jnp.int32)[None, :]).astype(jnp.int32)
    earlier = jnp.cumsum(hits, axis=0) - hits
    rank = jnp.sum(earlier * hits, axis=1)
    behind = (me - owner_of) % owners
    is_behind = (behind >= 1) & (behind <= reach)
    hop_of = jnp.where(is_behind, behind, (owners - behind) % owners)
    side_of = jnp.where(is_behind, 0, 1)
    share = cap // 2
    opposite = behind == reach
    side_of = jnp.where(opposite, jnp.where(rank < cap - share, 0, 1), side_of)
    rank = jnp.where(opposite & (side_of == 1), rank - (cap - share), rank)
    lane_of = hop_of * cap + rank
    place = (lane_of[None, :] == jnp.arange(slots, dtype=jnp.int32)[:, None]) & (
        side_of[None, :] == rep
    )

    def listed(values):
        return jnp.sum(jnp.where(place, values[None, :], jnp.zeros((), values.dtype)), axis=1)

    src = listed(jnp.arange(slot_count, dtype=jnp.int32))
    pair_at = listed(pair_of)
    tilt_at = listed(slot_tilt[0])
    focus = listed(defocus[0].astype(jnp.float32))
    pos_x = listed(slot_pos[0, 0].astype(jnp.float32))
    pos_y = listed(slot_pos[1, 0].astype(jnp.float32))
    valid = jnp.any(place, axis=1).astype(jnp.float32)

    peers = jnp.arange(owners, dtype=jnp.int32)
    hop_iota = jnp.arange(hops, dtype=jnp.int32)
    away = jnp.where(first, me - peers, peers - me) % owners
    pair_list = pair_at[:used].reshape(hops, cap).astype(jnp.float32)
    focus_list = focus[:used].reshape(hops, cap)
    near_hit = away[:, None] == hop_iota[None, :]
    far_hit = (away[:, None] + RADIUS == hop_iota[None, :]) & (away[:, None] >= 1)

    def rows_of(hit, table):
        return jnp.sum(jnp.where(hit[:, :, None], table[None], 0.0), axis=1)

    asked = jnp.concatenate(
        [rows_of(near_hit, pair_list), rows_of(near_hit, focus_list), rows_of(far_hit, pair_list)],
        axis=1,
    )
    heard = lax.all_to_all(asked, "dom", 0, 0, tiled=True)

    low_y = np.arange(half).astype(np.float32)
    freq_x = signed_freq(pixels)

    focus, pos_x, pos_y, tilt_at, src = (
        v + later.astype(v.dtype) for v in (focus, pos_x, pos_y, tilt_at, src)
    )
    weights = node_weights(pos_x, pos_y, GRID)
    tilt_match = tilt_at[:, None] == jnp.arange(tilt_dev, dtype=jnp.int32)[None, :]
    all_shift = jnp.dot(
        weights,
        warp_grid.reshape(tilt_dev * 2, node_count).T,
        precision=lax.Precision.HIGHEST,
        preferred_element_type=jnp.float32,
    ).reshape(slots, tilt_dev, 2)
    shifts = jnp.sum(jnp.where(tilt_match[:, :, None], all_shift, 0.0), axis=1)
    shift_x, shift_y = shifts[:, 0:1], shifts[:, 1:2]
    cos_table, sin_table = dft_tables(pixels)
    zeros = np.zeros((14, pixels), jnp.bfloat16)
    edge_rows = [cos_table[half : half + 1], sin_table[half : half + 1], zeros]
    row_table = jnp.asarray(np.concatenate([cos_table[:half], sin_table[:half]] + edge_rows, axis=0))
    side_table = jnp.asarray(np.concatenate(edge_rows, axis=0))
    col_table = jnp.asarray(np.concatenate([cos_table, sin_table], axis=1))
    qc, qs, pc, ps = contrast_tables(focus, low_y, freq_x, nyquist)
    angle_y, angle_x = turn * low_y[None] * shift_y, turn * freq_x[None] * shift_x
    row_tab = lane_tables([jnp.cos(angle_y), jnp.sin(angle_y), qc, qs], pixels)
    col_tab = jnp.stack([jnp.cos(angle_x), jnp.sin(angle_x), pc, ps], axis=0)

    total_groups = slots // GROUP
    part_groups = total_groups // 4
    parts = [(i * part_groups, part_groups if i < 3 else total_groups - 3 * part_groups) for i in range(4)]
    turned = []
    for start, number in parts:
        turned.append(
            spectra(
                src, patches[0], row_table, col_table, side_table, row_tab, col_tab, start, number
            )
        )
    edge = jnp.concatenate([t[3] for t in turned], axis=1)
    side_re = edge[2, :, :half] - edge[3, :, half:]
    side_im = -(edge[3, :, :half] + edge[2, :, half:])
    side_re = jnp.concatenate([side_re, side_re], axis=1)
    side_im = jnp.concatenate([side_im, -side_im], axis=1)
    side_y = np.concatenate([low_y, -low_y])
    edge_angle = turn * (freq_x[None] * shift_x - float(nyquist) * shift_y)
    side_angle = turn * (side_y[None] * shift_y - float(nyquist) * shift_x)
    edge_cos, edge_sin = jnp.cos(edge_angle), jnp.sin(edge_angle)
    side_cos, side_sin = jnp.cos(side_angle), jnp.sin(side_angle)
    line = jnp.stack(
        [
            edge[0] * edge_cos - edge[1] * edge_sin,
            edge[0] * edge_sin + edge[1] * edge_cos,
            contrast_of(focus[:, None], ((freq_x * freq_x + nyquist * nyquist) * scale_q)[None]),
            side_re * side_cos - side_im * side_sin,
            side_re * side_sin + side_im * side_cos,
            contrast_of(focus[:, None], ((side_y * side_y + nyquist * nyquist) * scale_q)[None]),
        ],
        axis=0,
    )

    since = jnp.where(first, peers - me, me - peers) % owners
    heard = rows_of((since[None, :] == hop_iota[:, None]), heard)
    asked_len = slots + GROUP
    asked_pair = jnp.pad(heard[:, :cap].reshape(-1).astype(jnp.int32), (0, asked_len - used))
    asked_focus = jnp.pad(heard[:, cap : 2 * cap].reshape(-1), (0, asked_len - used))
    far_count = reach - RADIUS
    far_pair = heard[1 : far_count + 1, 2 * cap :].reshape(-1).astype(jnp.int32)

    caps = (cap,) * (far_count - 1) + (cap - share,)
    sent = picked(far_pair, ring_blocks[RADIUS], counts, cap, caps)
    arrived = {}
    for j in range(far_count, 0, -1):
        arrived[RADIUS + j] = lax.ppermute(sent[j - 1], ("dom", "rep"), ring(j))

    aqc, aqs, apc, aps = contrast_tables(asked_focus, low_y, freq_x, nyquist)
    apart = apart_of(
        asked_pair, spreads, counts, lane_tables([aqc, aqs], pixels), jnp.stack([apc, aps], 0)
    )
    apart = jnp.sum(apart, axis=1)

    sums = []
    for (start, number), (re, im, ctf, _) in zip(parts, turned, strict=True):
        begin = start * GROUP // cap
        end = min((start + number) * GROUP // cap, hops)
        sources = [
            (ring_blocks[hop], counts, False) if hop <= RADIUS else ([arrived[hop]], (caps[hop - RADIUS - 1],), True)
            for hop in range(begin, end)
        ]
        rows = line[:, start * GROUP : (start + number) * GROUP]
        sums.append(terms_of(begin, pair_at, sources, (re, im, ctf, rows), cap))

    sums = jnp.concatenate(sums, axis=1)
    inverse_area = 1.0 / (pixels * pixels)
    energy = jnp.sum(sums[0], axis=1)
    grad_x = turn * jnp.sum(freq_x[None] * sums[1] - float(nyquist) * sums[3], axis=1)
    grad_y = turn * jnp.sum(sums[2], axis=1)
    per_slot = jnp.stack(
        [energy * inverse_area, 2.0 * inverse_area * grad_x, 2.0 * inverse_area * grad_y], axis=0
    )
    per_slot = jnp.where(valid[None, :used] > 0.0, per_slot, 0.0)

    spot = tilt_match.astype(jnp.float32)[:used].T[:, None, :]
    node_coef = (spot * per_slot[None, 1:3]).reshape(2 * tilt_dev, used)
    gradient = jnp.dot(
        node_coef,
        weights[:used],
        precision=lax.Precision.HIGHEST,
        preferred_element_type=jnp.float32,
    )
    own_terms = jnp.sum(jnp.where(place[None, :used], per_slot[:, :, None], 0.0), axis=1)
    answers = jnp.pad(apart, (0, node_count // 2 - asked_len))
    rep_row = jnp.arange(2, dtype=jnp.int32)[:, None] == rep
    answers = jnp.where(rep_row, answers[None, :], 0.0)
    gradient, own_terms, answers = lax.psum((gradient, own_terms, answers), "rep")
    bundle = jnp.concatenate([gradient, answers.reshape(1, node_count)], axis=0)
    near = 4
    blocks_of = [[near * i + j for j in range(near)] for i in range(owners // near)]
    strides_of = [[near * i + j for i in range(owners // near)] for j in range(near)]
    here = lax.all_gather(bundle, "dom", axis=0, axis_index_groups=blocks_of)
    bundle = jnp.concatenate(
        [jnp.sum(here[:, : 2 * tilt_dev], axis=0), here[:, 2 * tilt_dev]], axis=0
    )
    everyone = lax.all_gather(bundle, "dom", axis=0, axis_index_groups=strides_of)
    total = jnp.sum(everyone[:, : 2 * tilt_dev], axis=0).reshape(tilt_dev, 2, node_count)
    new_warp = warp_grid - total / jnp.sqrt(total * total + TRUST_FLOOR * TRUST_FLOOR)
    replies = everyone[:, 2 * tilt_dev :].reshape(owners, 2, node_count // 2)
    reply_hop = jnp.arange(node_count // 2, dtype=jnp.int32) // cap
    reply_owner = jnp.stack([me - reply_hop, me + reply_hop], axis=0) % owners
    reply = jnp.sum(jnp.where(peers[:, None, None] == reply_owner[None], replies, 0.0), axis=0)
    reply_lane = jnp.arange(node_count // 2, dtype=jnp.int32)
    reply_hit = (side_of[:, None, None] == jnp.arange(2, dtype=jnp.int32)[None, :, None]) & (
        lane_of[:, None, None] == reply_lane[None, None, :]
    )
    apart_own = jnp.sum(jnp.where(reply_hit, reply[None], 0.0), axis=(1, 2)) * inverse_area
    slot_terms = jnp.concatenate([own_terms[0:1] + apart_own[None], own_terms[1:]], axis=0)
    return (slot_terms[:, None, :], new_warp)


def solution(mesh):
    in_specs = (
        P(("groups", "tilt"), "dom", None, None),
        P(("groups", "tilt"), "dom", None),
        P(("groups", "tilt"), "dom"),
        P(None, ("groups", "tilt"), "dom"),
        P(("groups", "tilt"), "dom"),
        P(("groups", "dom"), "tilt", None, "rep", None),
        P(("groups", "tilt"), None, None),
    )
    out_specs = (P(None, ("groups", "tilt"), "dom"), P(("groups", "tilt"), None, None))

    return jax.shard_map(on_device, mesh=mesh, in_specs=in_specs, out_specs=out_specs, check_vma=False)
```

```python
import functools
import math

import jax
import jax.numpy as jnp
import numpy as np
from jax import lax
from jax.experimental import pallas as pl
from jax.experimental.pallas import tpu as pltpu
from jax.sharding import PartitionSpec as P


GRID = 16
AMPLITUDE = 0.07
TRUST_FLOOR = 0.02
RADIUS = 9
CHUNKS = 2
GROUP = 8
EXTRA = 4
BIG = math.sqrt(1.0 - AMPLITUDE * AMPLITUDE)


def signed_freq(pixels):
    index = np.arange(pixels)
    return np.where(index < pixels // 2, index, index - pixels).astype(np.float32)


def dft_tables(pixels):
    index = np.arange(pixels)
    angle = (index[:, None] * index[None, :] % pixels) * (2.0 * math.pi / pixels)
    scale = 1.0 / math.sqrt(pixels)
    return tuple(
        np.asarray(t * scale, np.float32).astype(jnp.bfloat16) for t in (np.cos(angle), np.sin(angle))
    )


def node_weights(pos_x, pos_y, grid_side):
    knot_pos = jnp.arange(grid_side, dtype=jnp.int32).astype(jnp.float32)
    weight_x = jnp.maximum(0.0, 1.0 - jnp.abs(pos_x[:, None] * (grid_side - 1) - knot_pos[None, :]))
    weight_y = jnp.maximum(0.0, 1.0 - jnp.abs(pos_y[:, None] * (grid_side - 1) - knot_pos[None, :]))
    return (weight_y[:, :, None] * weight_x[:, None, :]).reshape(
        pos_x.shape[0], grid_side * grid_side
    )


def iota(shape, dim):
    return lax.broadcasted_iota(jnp.int32, shape, dim)


def line_dot(a, b):
    return lax.dot_general(a, b, (((1,), (1,)), ((), ())), preferred_element_type=jnp.float32)


def fold_kernel(rep_ref, own_ref, recv_ref, out_ref, spread_ref):
    first = rep_ref[0] == 0
    views, tilts, half, pixels = own_ref.shape[0], own_ref.shape[1], own_ref.shape[3], own_ref.shape[4]
    flip_cols = ((iota((pixels, pixels), 0) + iota((pixels, pixels), 1)) % pixels == 0).astype(
        jnp.bfloat16
    )
    row_a, row_b = iota((2 * half, 2 * half), 0), iota((2 * half, 2 * half), 1)
    flip_rows = (
        (row_a // half == row_b // half) & (row_a % half + row_b % half == half)
    ).astype(jnp.bfloat16)
    at_edge = (iota((16, pixels), 1) == pixels // 2).astype(jnp.bfloat16)
    lane, line = iota((half, pixels), 1), iota((half, pixels), 0)
    whole = line == 0
    alone = jnp.logical_or(whole, lane == pixels // 2)
    count = views * tilts
    extras = []
    batch = 5
    for start in range(0, count, batch):
        lows, boths = [], []
        for p in range(start, start + batch):
            v, t = p // tilts, p % tilts
            own, recv = own_ref[v, t], recv_ref[v, t]
            lows.append(jnp.where(first, own, recv).reshape(2 * half, pixels))
            boths.append(jnp.where(first, recv, own).reshape(2 * half, pixels))
        turned = jnp.dot(
            jnp.concatenate(boths, axis=0), flip_cols, preferred_element_type=jnp.float32
        ).astype(jnp.bfloat16)
        mirrors = [
            jnp.dot(
                flip_rows,
                turned[2 * half * i : 2 * half * (i + 1)],
                preferred_element_type=jnp.float32,
            )
            for i in range(batch)
        ]
        cols = [
            line_dot(at_edge, jnp.concatenate([low, mirror.astype(jnp.bfloat16)], axis=0))
            for low, mirror in zip(lows, mirrors, strict=True)
        ]
        for i in range(batch):
            p = start + i
            low, mirror = lows[i].astype(jnp.float32), mirrors[i]
            low_re, low_im, mir_re, mir_im = low[:half], low[half:], mirror[:half], mirror[half:]
            base = p * 2 * half
            even_re = jnp.where(whole, low_re, 0.5 * (low_re + mir_re))
            even_im = jnp.where(whole, low_im, 0.5 * (low_im - mir_im))
            out_ref[base : base + half, :] = even_re.astype(jnp.bfloat16)
            out_ref[base + half : base + 2 * half, :] = even_im.astype(jnp.bfloat16)
            odd_re, odd_im = 0.5 * (low_re - mir_re), 0.5 * (low_im + mir_im)
            spread_ref[p] = jnp.where(alone, 0.0, 2.0 * (odd_re * odd_re + odd_im * odd_im))
            both = boths[i].astype(jnp.float32)
            col = cols[i][0:1]
            extras += [
                both[0:1],
                both[half : half + 1],
                jnp.concatenate([col[:, :half], col[:, 2 * half : 3 * half]], axis=1),
                jnp.concatenate([col[:, half : 2 * half], col[:, 3 * half :]], axis=1),
            ]
    top = count * 2 * half
    for g in range(count * EXTRA // 16):
        out_ref[top + 16 * g : top + 16 * (g + 1), :] = jnp.concatenate(
            extras[16 * g : 16 * (g + 1)], axis=0
        ).astype(jnp.bfloat16)


def folded(own, recv, rep_index, chunk):
    views, tilts, _, half, pixels = own.shape
    per = views // CHUNKS
    count = per * tilts
    rows = count * (2 * half + EXTRA)
    return pl.pallas_call(
        fold_kernel,
        grid=(1,),
        in_specs=[
            pl.BlockSpec(memory_space=pltpu.SMEM),
            pl.BlockSpec((per, tilts, 2, half, pixels), lambda v: (chunk, 0, 0, 0, 0)),
            pl.BlockSpec((per, tilts, 2, half, pixels), lambda v: (chunk, 0, 0, 0, 0)),
        ],
        out_specs=[
            pl.BlockSpec((rows, pixels), lambda v: (0, 0)),
            pl.BlockSpec((count, half, pixels), lambda v: (0, 0, 0)),
        ],
        out_shape=[
            jax.ShapeDtypeStruct((rows, pixels), jnp.bfloat16),
            jax.ShapeDtypeStruct((count, half, pixels), jnp.float32),
        ],
        name="fold",
    )(rep_index, own, recv)


def dft_kernel(src_ref, patch_ref, row_ref, col_ref, side_ref, rt_ref, ct_ref, *outs, start):
    out_re, out_im, out_ctf, edge_ref = outs
    step = pl.program_id(0) + start
    pixels = col_ref.shape[0]
    half = pixels // 2
    rt = rt_ref[0]
    firsts = [
        jnp.dot(
            row_ref[...], patch_ref[src_ref[step * GROUP + k]], preferred_element_type=jnp.float32
        ).astype(jnp.bfloat16)
        for k in range(GROUP)
    ]
    boths = [jnp.dot(f, col_ref[...], preferred_element_type=jnp.float32) for f in firsts]
    sides = [line_dot(side_ref[...], f[:pixels]) for f in firsts]
    for k in range(GROUP):
        both, side = boths[k], sides[k]
        re = both[:half, :pixels] - both[half:pixels, pixels:]
        im = -(both[:half, pixels:] + both[half:pixels, :pixels])
        cy, sy = rt[:, k : k + 1], rt[:, GROUP + k : GROUP + k + 1]
        qc = rt[:, 2 * GROUP + k : 2 * GROUP + k + 1]
        qs = rt[:, 3 * GROUP + k : 3 * GROUP + k + 1]
        cx, sx, pc, ps = (ct_ref[i, k : k + 1, :] for i in range(4))
        er = cy * cx - sy * sx
        ei = sy * cx + cy * sx
        out_re[k] = re * er - im * ei
        out_im[k] = re * ei + im * er
        out_ctf[k] = qc * pc + qs * ps
        low, high = both[pixels : pixels + 1], both[pixels + 1 : pixels + 2]
        edge_ref[0, k : k + 1, :] = low[:, :pixels] - high[:, pixels:]
        edge_ref[1, k : k + 1, :] = -(low[:, pixels:] + high[:, :pixels])
        edge_ref[2, k : k + 1, :] = side[0:1]
        edge_ref[3, k : k + 1, :] = side[1:2]


def spectra(src, patches, row_table, col_table, side_table, row_tab, col_tab, start, groups):
    _, half, pixels = row_tab.shape
    slots = groups * GROUP
    tall = row_table.shape[0]
    plane = pl.BlockSpec((GROUP, half, pixels), lambda g: (g, 0, 0))
    shape = jax.ShapeDtypeStruct((slots, half, pixels), jnp.float32)
    return pl.pallas_call(
        functools.partial(dft_kernel, start=start),
        grid=(groups,),
        in_specs=[
            pl.BlockSpec(memory_space=pltpu.SMEM),
            pl.BlockSpec(patches.shape, lambda g: (0, 0, 0)),
            pl.BlockSpec((tall, pixels), lambda g: (0, 0)),
            pl.BlockSpec((pixels, 2 * pixels), lambda g: (0, 0)),
            pl.BlockSpec(side_table.shape, lambda g: (0, 0)),
            pl.BlockSpec((1, half, pixels), lambda g: (g + start, 0, 0)),
            pl.BlockSpec((4, GROUP, pixels), lambda g: (0, g + start, 0)),
        ],
        out_specs=[plane, plane, plane, pl.BlockSpec((4, GROUP, pixels), lambda g: (0, g, 0))],
        out_shape=[shape, shape, shape, jax.ShapeDtypeStruct((4, slots, pixels), jnp.float32)],
        cost_estimate=pl.CostEstimate(flops=10**9 * groups, bytes_accessed=2 * 10**7, transcendentals=0),
        name="spectra",
    )(src, patches, row_table, col_table, side_table, row_tab, col_tab)


def chosen(refs, pair, start, size, stride):
    per = refs[0][1]
    rows = None
    for i, (ref, count) in enumerate(refs):
        q = jnp.clip(pair - i * per, 0, count - 1)
        at = pl.multiple_of(start(count, q), stride)
        part = ref[pl.ds(at, size), :]
        rows = part if rows is None else jnp.where(pair >= i * per, part, rows)
    return rows


def extra_rows(refs, pair, pixels):
    return chosen(refs, pair, lambda n, q: n * pixels + (q // 4) * 16, 16, 16)


def terms_kernel(ids_ref, *refs, sources, base, cap):
    at, held_by = 0, []
    for counts, _ in sources:
        held_by.append(list(zip(refs[at : at + len(counts)], counts, strict=True)))
        at += len(counts)
    re_ref, im_ref, ctf_ref, line_ref, out_ref = refs[at:]
    _, half, pixels = re_ref.shape
    line, lane = iota((half, pixels), 0), iota((half, pixels), 1)
    weight = jnp.where(line == 0, 1.0, jnp.where(lane == half, 0.0, 2.0))
    fy = line.astype(jnp.float32)
    edge = iota((1, pixels), 1)
    col_weight = jnp.where(edge % half == 0, 0.0, 1.0)
    col_fy = jnp.where(edge < half, edge, half - edge).astype(jnp.float32)
    for n, (counts, fixed) in enumerate(sources):
        held = held_by[n]
        for k in range(cap):
            i = n * cap + k
            pair = jnp.int32(k) if fixed else ids_ref[base + i]
            ref_blk = chosen(held, pair, lambda m, q: q * pixels, pixels, pixels).astype(jnp.float32)
            group = extra_rows(held, pair, pixels)
            picker = iota((8, 16), 1) == 4 * ((pair % counts[0]) % 4) + iota((8, 16), 0)
            rim = jnp.dot(picker.astype(jnp.bfloat16), group, preferred_element_type=jnp.float32)
            ctf = ctf_ref[i]
            mod_re, mod_im = ctf * ref_blk[:half], ctf * ref_blk[half:]
            dif_re, dif_im = re_ref[i] - mod_re, im_ref[i] - mod_im
            power = weight * (dif_re * dif_re + dif_im * dif_im)
            cross = weight * (dif_im * mod_re - dif_re * mod_im)
            own = [line_ref[j, i : i + 1, :] for j in range(6)]

            def edge_terms(a, b, own=own, rim=rim):
                m_re, m_im = own[a + 2] * rim[b : b + 1], own[a + 2] * rim[b + 1 : b + 2]
                d_re, d_im = own[a] - m_re, own[a + 1] - m_im
                return d_re * d_re + d_im * d_im, d_im * m_re - d_re * m_im

            row_power, row_cross = edge_terms(0, 0)
            col_power, col_cross = edge_terms(3, 2)
            col_cross = col_weight * col_cross
            out_ref[0, i : i + 1, :] = (
                jnp.sum(power, axis=0, keepdims=True) + row_power + col_weight * col_power
            )
            out_ref[1, i : i + 1, :] = jnp.sum(cross, axis=0, keepdims=True) + row_cross
            out_ref[2, i : i + 1, :] = (
                jnp.sum(fy * cross, axis=0, keepdims=True) - half * row_cross + col_fy * col_cross
            )
            out_ref[3, i : i + 1, :] = col_cross


def terms_of(first_hop, ids, sources, turned, cap):
    re, im, ctf, line = turned
    _, half, pixels = re.shape
    number = len(sources) * cap
    arrays = [a for blocks, _, _ in sources for a in blocks]
    plane = pl.BlockSpec((number, half, pixels), lambda g: (0, 0, 0))
    return pl.pallas_call(
        functools.partial(
            terms_kernel, sources=[(c, f) for _, c, f in sources], base=first_hop * cap, cap=cap
        ),
        grid=(1,),
        in_specs=[pl.BlockSpec(memory_space=pltpu.SMEM)]
        + [pl.BlockSpec(a.shape, lambda g: (0, 0)) for a in arrays]
        + [plane, plane, plane, pl.BlockSpec(line.shape, lambda g: (0, 0, 0))],
        out_specs=pl.BlockSpec((4, number, pixels), lambda g: (0, 0, 0)),
        out_shape=jax.ShapeDtypeStruct((4, number, pixels), jnp.float32),
        cost_estimate=pl.CostEstimate(flops=10**9, bytes_accessed=10**7, transcendentals=0),
        name="terms",
    )(ids, *arrays, re, im, ctf, line)


def pick_kernel(ids_ref, *refs, counts, cap, caps):
    held = list(zip(refs[: len(counts)], counts, strict=True))
    pixels = refs[0].shape[1]
    for j, out in enumerate(refs[len(counts) :]):
        groups = [None] * (-(-caps[j] * EXTRA // 16))
        for k in range(caps[j]):
            pair = ids_ref[j * cap + k]
            out[k * pixels : (k + 1) * pixels, :] = chosen(
                held, pair, lambda n, q: q * pixels, pixels, pixels
            )
            group = extra_rows(held, pair, pixels)
            row, col = iota((16, 16), 0), iota((16, 16), 1)
            mover = (row // 4 == k % 4) & (col // 4 == (pair % counts[0]) % 4) & (row % 4 == col % 4)
            moved = jnp.dot(mover.astype(jnp.bfloat16), group, preferred_element_type=jnp.float32)
            g = k // 4
            groups[g] = moved if groups[g] is None else groups[g] + moved
        for g, rows in enumerate(groups):
            at = caps[j] * pixels + 16 * g
            out[at : at + 16, :] = rows.astype(jnp.bfloat16)


def picked(ids, blocks, counts, cap, caps):
    pixels = blocks[0].shape[1]
    rows = [c * pixels + 16 * (-(-c * EXTRA // 16)) for c in caps]
    return pl.pallas_call(
        functools.partial(pick_kernel, counts=counts, cap=cap, caps=caps),
        grid=(1,),
        in_specs=[pl.BlockSpec(memory_space=pltpu.SMEM)]
        + [pl.BlockSpec(b.shape, lambda g: (0, 0)) for b in blocks],
        out_specs=[pl.BlockSpec((r, pixels), lambda g: (0, 0)) for r in rows],
        out_shape=[jax.ShapeDtypeStruct((r, pixels), jnp.bfloat16) for r in rows],
        name="pick",
    )(ids, *blocks)


def apart_kernel(ids_ref, *refs, counts):
    held = refs[: len(counts)]
    rt_ref, ct_ref, out_ref = refs[len(counts) :]
    step = pl.program_id(0)
    rt = rt_ref[0]
    for k in range(GROUP):
        pair = ids_ref[step * GROUP + k]
        power = None
        for i, (ref, count) in enumerate(zip(held, counts, strict=True)):
            part = ref[jnp.clip(pair - i * counts[0], 0, count - 1)]
            power = part if power is None else jnp.where(pair >= i * counts[0], part, power)
        ctf = (
            rt[:, k : k + 1] * ct_ref[0, k : k + 1, :]
            + rt[:, GROUP + k : GROUP + k + 1] * ct_ref[1, k : k + 1, :]
        )
        out_ref[k : k + 1, :] = jnp.sum(ctf * ctf * power, axis=0, keepdims=True)


def apart_of(ids, spreads, counts, row_tab, col_tab):
    groups, half, pixels = row_tab.shape
    return pl.pallas_call(
        functools.partial(apart_kernel, counts=counts),
        grid=(groups,),
        in_specs=[pl.BlockSpec(memory_space=pltpu.SMEM)]
        + [pl.BlockSpec(s.shape, lambda g: (0, 0, 0)) for s in spreads]
        + [
            pl.BlockSpec((1, half, pixels), lambda g: (g, 0, 0)),
            pl.BlockSpec((2, GROUP, pixels), lambda g: (0, g, 0)),
        ],
        out_specs=pl.BlockSpec((GROUP, pixels), lambda g: (g, 0)),
        out_shape=jax.ShapeDtypeStruct((groups * GROUP, pixels), jnp.float32),
        cost_estimate=pl.CostEstimate(flops=10**9, bytes_accessed=4 * 10**6, transcendentals=0),
        name="apart",
    )(ids, *spreads, row_tab, col_tab)


def lane_tables(tables, pixels):
    stacked = jnp.stack(tables, axis=0)
    count, slots, rows = stacked.shape
    laid = stacked.reshape(count, slots // GROUP, GROUP, rows).transpose(1, 3, 0, 2)
    laid = laid.reshape(slots // GROUP, rows, count * GROUP)
    return jnp.pad(laid, ((0, 0), (0, 0), (0, pixels - count * GROUP)))


def contrast_tables(focus, low_y, freq_x, nyquist):
    rate = math.pi * focus[:, None] / (nyquist * nyquist)
    by, bx = rate * (low_y * low_y)[None], rate * (freq_x * freq_x)[None]
    sin_x, cos_x = jnp.sin(bx), jnp.cos(bx)
    pc = -(BIG * sin_x + AMPLITUDE * cos_x)
    ps = -(BIG * cos_x - AMPLITUDE * sin_x)
    return jnp.cos(by), jnp.sin(by), pc, ps


def contrast_of(focus, radius):
    aberration = math.pi * focus * radius
    return -(BIG * jnp.sin(aberration) + AMPLITUDE * jnp.cos(aberration))


def on_device(patches, slot_view, slot_tilt, slot_pos, defocus, projections, warp_grid):
    owners = lax.axis_size("dom")
    me = lax.axis_index("dom")
    rep = lax.axis_index("rep")
    first = rep == 0
    slot_count = patches.shape[1]
    pixels = patches.shape[-1]
    half = nyquist = pixels // 2
    view_dev = projections.shape[0]
    tilt_dev = warp_grid.shape[0]
    node_count = warp_grid.shape[2]
    pair_dev = view_dev * tilt_dev
    cap = 3 * slot_count // (2 * owners)
    reach = owners // 2
    hops = reach + 1
    used = hops * cap
    slots = -(-used // GROUP) * GROUP
    counts = (pair_dev // CHUNKS,) * CHUNKS
    turn = 2.0 * math.pi / pixels
    scale_q = 1.0 / (nyquist * nyquist)

    recv = lax.ppermute(projections, "rep", [(0, 1), (1, 0)])
    rep_index = jnp.reshape(rep, (1,)).astype(jnp.int32)
    made = []
    for c in range(CHUNKS):
        made.append(folded(projections, recv, rep_index, c))
    blocks = [m[0] for m in made]
    spreads = [m[1] for m in made]

    def ring(shift):
        pairs = []
        for i in range(owners):
            pairs.append((2 * i, 2 * ((i + shift) % owners)))
            pairs.append((2 * i + 1, 2 * ((i - shift) % owners) + 1))
        return pairs

    ring_blocks = [blocks]
    for _ in range(1, RADIUS + 1):
        sent = []
        for block in ring_blocks[-1]:
            sent.append(lax.ppermute(block, ("dom", "rep"), ring(1)))
        ring_blocks.append(sent)

    later = made[-1][1][0, 0, 0].astype(jnp.int32)

    chosen_view = slot_view[0, :, 0]
    owner_of = chosen_view // view_dev
    pair_of = (chosen_view % view_dev) * tilt_dev + slot_tilt[0]
    hits = (owner_of[:, None] == jnp.arange(owners, dtype=jnp.int32)[None, :]).astype(jnp.int32)
    earlier = jnp.cumsum(hits, axis=0) - hits
    rank = jnp.sum(earlier * hits, axis=1)
    behind = (me - owner_of) % owners
    is_behind = (behind >= 1) & (behind <= reach)
    hop_of = jnp.where(is_behind, behind, (owners - behind) % owners)
    side_of = jnp.where(is_behind, 0, 1)
    share = cap // 2
    opposite = behind == reach
    side_of = jnp.where(opposite, jnp.where(rank < cap - share, 0, 1), side_of)
    rank = jnp.where(opposite & (side_of == 1), rank - (cap - share), rank)
    lane_of = hop_of * cap + rank
    place = (lane_of[None, :] == jnp.arange(slots, dtype=jnp.int32)[:, None]) & (
        side_of[None, :] == rep
    )

    def listed(values):
        return jnp.sum(jnp.where(place, values[None, :], jnp.zeros((), values.dtype)), axis=1)

    src = listed(jnp.arange(slot_count, dtype=jnp.int32))
    pair_at = listed(pair_of)
    tilt_at = listed(slot_tilt[0])
    focus = listed(defocus[0].astype(jnp.float32))
    pos_x = listed(slot_pos[0, 0].astype(jnp.float32))
    pos_y = listed(slot_pos[1, 0].astype(jnp.float32))
    valid = jnp.any(place, axis=1).astype(jnp.float32)

    peers = jnp.arange(owners, dtype=jnp.int32)
    hop_iota = jnp.arange(hops, dtype=jnp.int32)
    away = jnp.where(first, me - peers, peers - me) % owners
    pair_list = pair_at[:used].reshape(hops, cap).astype(jnp.float32)
    focus_list = focus[:used].reshape(hops, cap)
    near_hit = away[:, None] == hop_iota[None, :]
    far_hit = (away[:, None] + RADIUS == hop_iota[None, :]) & (away[:, None] >= 1)

    def rows_of(hit, table):
        return jnp.sum(jnp.where(hit[:, :, None], table[None], 0.0), axis=1)

    asked = jnp.concatenate(
        [rows_of(near_hit, pair_list), rows_of(near_hit, focus_list), rows_of(far_hit, pair_list)],
        axis=1,
    )
    heard = lax.all_to_all(asked, "dom", 0, 0, tiled=True)

    low_y = np.arange(half).astype(np.float32)
    freq_x = signed_freq(pixels)

    focus, pos_x, pos_y, tilt_at, src = (
        v + later.astype(v.dtype) for v in (focus, pos_x, pos_y, tilt_at, src)
    )
    weights = node_weights(pos_x, pos_y, GRID)
    tilt_match = tilt_at[:, None] == jnp.arange(tilt_dev, dtype=jnp.int32)[None, :]
    all_shift = jnp.dot(
        weights,
        warp_grid.reshape(tilt_dev * 2, node_count).T,
        precision=lax.Precision.HIGHEST,
        preferred_element_type=jnp.float32,
    ).reshape(slots, tilt_dev, 2)
    shifts = jnp.sum(jnp.where(tilt_match[:, :, None], all_shift, 0.0), axis=1)
    shift_x, shift_y = shifts[:, 0:1], shifts[:, 1:2]
    cos_table, sin_table = dft_tables(pixels)
    zeros = np.zeros((14, pixels), jnp.bfloat16)
    edge_rows = [cos_table[half : half + 1], sin_table[half : half + 1], zeros]
    row_table = jnp.asarray(np.concatenate([cos_table[:half], sin_table[:half]] + edge_rows, axis=0))
    side_table = jnp.asarray(np.concatenate(edge_rows, axis=0))
    col_table = jnp.asarray(np.concatenate([cos_table, sin_table], axis=1))
    qc, qs, pc, ps = contrast_tables(focus, low_y, freq_x, nyquist)
    angle_y, angle_x = turn * low_y[None] * shift_y, turn * freq_x[None] * shift_x
    row_tab = lane_tables([jnp.cos(angle_y), jnp.sin(angle_y), qc, qs], pixels)
    col_tab = jnp.stack([jnp.cos(angle_x), jnp.sin(angle_x), pc, ps], axis=0)

    total_groups = slots // GROUP
    part_groups = total_groups // 4
    parts = [(i * part_groups, part_groups if i < 3 else total_groups - 3 * part_groups) for i in range(4)]
    turned = []
    for start, number in parts:
        turned.append(
            spectra(
                src, patches[0], row_table, col_table, side_table, row_tab, col_tab, start, number
            )
        )
    edge = jnp.concatenate([t[3] for t in turned], axis=1)
    side_re = edge[2, :, :half] - edge[3, :, half:]
    side_im = -(edge[3, :, :half] + edge[2, :, half:])
    side_re = jnp.concatenate([side_re, side_re], axis=1)
    side_im = jnp.concatenate([side_im, -side_im], axis=1)
    side_y = np.concatenate([low_y, -low_y])
    edge_angle = turn * (freq_x[None] * shift_x - float(nyquist) * shift_y)
    side_angle = turn * (side_y[None] * shift_y - float(nyquist) * shift_x)
    edge_cos, edge_sin = jnp.cos(edge_angle), jnp.sin(edge_angle)
    side_cos, side_sin = jnp.cos(side_angle), jnp.sin(side_angle)
    line = jnp.stack(
        [
            edge[0] * edge_cos - edge[1] * edge_sin,
            edge[0] * edge_sin + edge[1] * edge_cos,
            contrast_of(focus[:, None], ((freq_x * freq_x + nyquist * nyquist) * scale_q)[None]),
            side_re * side_cos - side_im * side_sin,
            side_re * side_sin + side_im * side_cos,
            contrast_of(focus[:, None], ((side_y * side_y + nyquist * nyquist) * scale_q)[None]),
        ],
        axis=0,
    )

    since = jnp.where(first, peers - me, me - peers) % owners
    heard = rows_of((since[None, :] == hop_iota[:, None]), heard)
    asked_len = slots + GROUP
    asked_pair = jnp.pad(heard[:, :cap].reshape(-1).astype(jnp.int32), (0, asked_len - used))
    asked_focus = jnp.pad(heard[:, cap : 2 * cap].reshape(-1), (0, asked_len - used))
    far_count = reach - RADIUS
    far_pair = heard[1 : far_count + 1, 2 * cap :].reshape(-1).astype(jnp.int32)

    caps = (cap,) * (far_count - 1) + (cap - share,)
    sent = picked(far_pair, ring_blocks[RADIUS], counts, cap, caps)
    arrived = {}
    for j in range(far_count, 0, -1):
        arrived[RADIUS + j] = lax.ppermute(sent[j - 1], ("dom", "rep"), ring(j))

    aqc, aqs, apc, aps = contrast_tables(asked_focus, low_y, freq_x, nyquist)
    apart = apart_of(
        asked_pair, spreads, counts, lane_tables([aqc, aqs], pixels), jnp.stack([apc, aps], 0)
    )
    apart = jnp.sum(apart, axis=1)

    sums = []
    for (start, number), (re, im, ctf, _) in zip(parts, turned, strict=True):
        begin = start * GROUP // cap
        end = min((start + number) * GROUP // cap, hops)
        sources = [
            (ring_blocks[hop], counts, False) if hop <= RADIUS else ([arrived[hop]], (caps[hop - RADIUS - 1],), True)
            for hop in range(begin, end)
        ]
        rows = line[:, start * GROUP : (start + number) * GROUP]
        sums.append(terms_of(begin, pair_at, sources, (re, im, ctf, rows), cap))

    sums = jnp.concatenate(sums, axis=1)
    inverse_area = 1.0 / (pixels * pixels)
    energy = jnp.sum(sums[0], axis=1)
    grad_x = turn * jnp.sum(freq_x[None] * sums[1] - float(nyquist) * sums[3], axis=1)
    grad_y = turn * jnp.sum(sums[2], axis=1)
    per_slot = jnp.stack(
        [energy * inverse_area, 2.0 * inverse_area * grad_x, 2.0 * inverse_area * grad_y], axis=0
    )
    per_slot = jnp.where(valid[None, :used] > 0.0, per_slot, 0.0)

    spot = tilt_match.astype(jnp.float32)[:used].T[:, None, :]
    node_coef = (spot * per_slot[None, 1:3]).reshape(2 * tilt_dev, used)
    gradient = jnp.dot(
        node_coef,
        weights[:used],
        precision=lax.Precision.HIGHEST,
        preferred_element_type=jnp.float32,
    )
    own_terms = jnp.sum(jnp.where(place[None, :used], per_slot[:, :, None], 0.0), axis=1)
    answers = jnp.pad(apart, (0, node_count // 2 - asked_len))
    rep_row = jnp.arange(2, dtype=jnp.int32)[:, None] == rep
    answers = jnp.where(rep_row, answers[None, :], 0.0)
    gradient, own_terms, answers = lax.psum((gradient, own_terms, answers), "rep")
    bundle = jnp.concatenate([gradient, answers.reshape(1, node_count)], axis=0)
    near = 4
    blocks_of = [[near * i + j for j in range(near)] for i in range(owners // near)]
    strides_of = [[near * i + j for i in range(owners // near)] for j in range(near)]
    here = lax.all_gather(bundle, "dom", axis=0, axis_index_groups=blocks_of)
    bundle = jnp.concatenate(
        [jnp.sum(here[:, : 2 * tilt_dev], axis=0), here[:, 2 * tilt_dev]], axis=0
    )
    everyone = lax.all_gather(bundle, "dom", axis=0, axis_index_groups=strides_of)
    total = jnp.sum(everyone[:, : 2 * tilt_dev], axis=0).reshape(tilt_dev, 2, node_count)
    new_warp = warp_grid - total / jnp.sqrt(total * total + TRUST_FLOOR * TRUST_FLOOR)
    replies = everyone[:, 2 * tilt_dev :].reshape(owners, 2, node_count // 2)
    reply_hop = jnp.arange(node_count // 2, dtype=jnp.int32) // cap
    reply_owner = jnp.stack([me - reply_hop, me + reply_hop], axis=0) % owners
    reply = jnp.sum(jnp.where(peers[:, None, None] == reply_owner[None], replies, 0.0), axis=0)
    reply_lane = jnp.arange(node_count // 2, dtype=jnp.int32)
    reply_hit = (side_of[:, None, None] == jnp.arange(2, dtype=jnp.int32)[None, :, None]) & (
        lane_of[:, None, None] == reply_lane[None, None, :]
    )
    apart_own = jnp.sum(jnp.where(reply_hit, reply[None], 0.0), axis=(1, 2)) * inverse_area
    slot_terms = jnp.concatenate([own_terms[0:1] + apart_own[None], own_terms[1:]], axis=0)
    return (slot_terms[:, None, :], new_warp)


def solution(mesh):
    in_specs = (
        P(("groups", "tilt"), "dom", None, None),
        P(("groups", "tilt"), "dom", None),
        P(("groups", "tilt"), "dom"),
        P(None, ("groups", "tilt"), "dom"),
        P(("groups", "tilt"), "dom"),
        P(("groups", "dom"), "tilt", None, "rep", None),
        P(("groups", "tilt"), None, None),
    )
    out_specs = (P(None, ("groups", "tilt"), "dom"), P(("groups", "tilt"), None, None))

    return jax.shard_map(on_device, mesh=mesh, in_specs=in_specs, out_specs=out_specs, check_vma=False)
```
